32 devices in a mesh: blk: 4 (over x, core), group: 8 (over z, y).
Axes of the slice: x: 2, y: 2, z: 4, core: 2. Of those that a mesh axis runs over, the one named last changes fastest.
Arguments:
- queries: bfloat16 [8, 512, 2048], P('group', 'blk'), may hold values from -300 to 300
- normed: bfloat16 [8, 512, 2048], P('group', 'blk'), may hold values from -6 to 6
- key_weight_copies: bfloat16 [8, 2048, 512], P('group', 'blk'), may hold values from -0.125 to 0.125
- value_weight_copies: bfloat16 [8, 2048, 512], P('group', 'blk'), may hold values from -0.125 to 0.125
- owner: int32 [4], replicated, may hold values from 0 to 7
Outputs:
- cache_keys: bfloat16 [8, 512, 512], P('group', 'blk')
- cache_values: bfloat16 [8, 512, 512], P('group', 'blk')
- attended: bfloat16 [8, 512, 2048], P('group', 'blk')
The draws below stay inside these ranges and needn't reach their ends.
Inputs may be any that keep to these rules, and one draw needn't show every extreme that they name: `owner`: learner group index of each block of projection rows, below the number of actor groups.
All inputs are finite; a program needn't handle non-finite values.
Results may differ from the reference program's by a relative error of at most 0.011.
Values may be sent and summed in bfloat16 or wider, within the bound.
A program may use at most 64 MiB of HBM per device.

```python
import math
import jax
import jax.numpy as jnp
from jax import lax

INPUT_FEATURES = 2048
QUERY_HEADS = 16
KEY_VALUE_HEADS = 4
HEAD_SIZE = 128
PROMPT_TOKENS = 512
ACTOR_GROUPS = 8
N_BLK = 4
N_GROUP = 8


def draw_queries(key, part):
    base_draw = jax.random.normal(jax.random.fold_in(key, 11), (ACTOR_GROUPS, PROMPT_TOKENS, QUERY_HEADS * HEAD_SIZE), jnp.float32)
    return jnp.clip(base_draw, -6.0, 6.0).astype(jnp.bfloat16)


def place_ends(entries, own_key, least, largest):
    extent = entries.shape
    spot = [jax.random.randint(jax.random.fold_in(own_key, axis), (), 0, extent[axis]) for axis in range(len(extent))]
    entries = entries.at[tuple(spot)].set(least)
    longest = extent.index(max(extent))
    spot[longest] = (spot[longest] + 1) % extent[longest]
    return entries.at[tuple(spot)].set(largest)


def level_of(stream_key, extent, shards, smallest, top_value):
    factor_of, own = 1.0, jax.random.fold_in(stream_key, 6)
    for position, blocks in shards:
        draws = jnp.exp(jax.random.uniform(jax.random.fold_in(own, position), (blocks,), jnp.float32, smallest / len(shards), top_value / len(shards)))
        factor_of = factor_of * jnp.repeat(draws, extent[position] // blocks).reshape([-1 if axis == position else 1 for axis in range(len(extent))])
    return factor_of


def scatter_about(stream_key, shape, width, limit, cuts=(), kind=jnp.bfloat16):
    factor_of = level_of(stream_key, shape, cuts, -0.22, 0.18) if cuts else 1.0
    result = jax.random.normal(stream_key, shape, jnp.float32) * width * factor_of
    return jnp.minimum(jnp.maximum(result, -limit), limit).astype(kind)


def setup_inputs(seed: int = 0) -> dict:
    seeds = jax.random.split(jax.random.key(seed), 6)
    return {
        "queries": draw_queries(jax.random.fold_in(seeds[5], 71), 0),
        "normed": scatter_about(seeds[1], (ACTOR_GROUPS, PROMPT_TOKENS, INPUT_FEATURES), 1.0, 6.0, ((0, 8), (1, 4))),
        "key_weight_copies": scatter_about(seeds[2], (ACTOR_GROUPS, INPUT_FEATURES, KEY_VALUE_HEADS * HEAD_SIZE), INPUT_FEATURES ** -0.5, 0.125, ((0, 8), (1, 4))),
        "value_weight_copies": scatter_about(seeds[3], (ACTOR_GROUPS, INPUT_FEATURES, KEY_VALUE_HEADS * HEAD_SIZE), INPUT_FEATURES ** -0.5, 0.125, ((0, 8), (1, 4))),
        "owner": place_ends(jax.random.randint(seeds[4], (N_BLK,), 0, N_GROUP), jax.random.fold_in(seeds[4], 1), 0, N_GROUP - 1).astype(jnp.int32),
    }


def rotate(unshaped_rows, positions):
    half_dim = HEAD_SIZE // 2
    inverse_freq = jnp.exp(jnp.arange(half_dim).astype(jnp.float32) * (-2.0 * math.log(500000.0) / HEAD_SIZE))
    angles = positions.astype(jnp.float32)[:, None] * inverse_freq[None, :]
    cos_table = jnp.cos(angles)[:, None, :]
    sin_table = jnp.sin(angles)[:, None, :]
    reshaped_rows = unshaped_rows.reshape(unshaped_rows.shape[0], KEY_VALUE_HEADS, HEAD_SIZE)
    first_half = reshaped_rows[..., :half_dim]
    second_half = reshaped_rows[..., half_dim:]
    transposed_rows = jnp.concatenate([first_half * cos_table - second_half * sin_table, second_half * cos_table + first_half * sin_table], axis=-1)
    return transposed_rows.reshape(unshaped_rows.shape[0], KEY_VALUE_HEADS * HEAD_SIZE)


def pick_rows(copies, owner):
    block_rows = INPUT_FEATURES // N_BLK
    blocked = copies.reshape(ACTOR_GROUPS, N_BLK, block_rows, copies.shape[2])
    chosen = blocked[owner.astype(jnp.int32), jnp.arange(N_BLK, dtype=jnp.int32)]
    return chosen.reshape(INPUT_FEATURES, copies.shape[2])


def reference(queries, normed, key_weight_copies, value_weight_copies, owner):
    key_proj = pick_rows(key_weight_copies, owner)
    value_proj = pick_rows(value_weight_copies, owner)
    positions = jnp.arange(PROMPT_TOKENS)
    allowed = positions[None, :] <= positions[:, None]

    def per_actor(actor_pair):
        projected_query_rows, input_rows = actor_pair
        layer_key_cache = rotate(jnp.dot(input_rows, key_proj, preferred_element_type=jnp.float32), positions).astype(jnp.bfloat16)
        value_rows = jnp.dot(input_rows, value_proj, preferred_element_type=jnp.float32).astype(jnp.bfloat16)
        query_head_grid = projected_query_rows.reshape(PROMPT_TOKENS, KEY_VALUE_HEADS, QUERY_HEADS // KEY_VALUE_HEADS, HEAD_SIZE).astype(jnp.float32)
        full_score_matrix = jnp.einsum('lewc,jec->ewlj', query_head_grid, layer_key_cache.reshape(PROMPT_TOKENS, KEY_VALUE_HEADS, HEAD_SIZE).astype(jnp.float32)) * (HEAD_SIZE ** -0.5)
        full_score_matrix = jnp.where(allowed, full_score_matrix, -jnp.inf)
        row_max = jnp.max(full_score_matrix, axis=-1, keepdims=True)
        full_probabilities = jnp.exp(full_score_matrix - row_max)
        row_total = jnp.sum(full_probabilities, axis=-1)
        weighted_values = jnp.einsum('lxbp,plj->lxbj', full_probabilities.astype(jnp.bfloat16).astype(jnp.float32), value_rows.reshape(PROMPT_TOKENS, KEY_VALUE_HEADS, HEAD_SIZE).astype(jnp.float32))
        mixed_out = weighted_values / row_total[..., None]
        attended = mixed_out.transpose(2, 0, 1, 3).reshape(PROMPT_TOKENS, QUERY_HEADS * HEAD_SIZE).astype(jnp.bfloat16)
        return layer_key_cache, value_rows, attended

    cache_keys, cache_values, attended = lax.map(per_actor, (queries, normed))
    return cache_keys, cache_values, attended
```

```python
import functools
import math

import jax
import jax.numpy as jnp
from jax import lax
from jax.experimental import pallas as pl
from jax.experimental.pallas import tpu as pltpu
from jax.sharding import PartitionSpec as P

QUERY_HEADS = 16
KEY_VALUE_HEADS = 4
HEAD_SIZE = 128
MESH = pl.DeviceIdType.MESH


def spread(value, axis, source):
    kept = jnp.where(lax.axis_index(axis) == source, value, 0).astype(value.dtype)
    return lax.psum(kept, axis)


def rotate(unshaped_rows, positions):
    half_dim = HEAD_SIZE // 2
    inverse_freq = jnp.exp(
        jnp.arange(half_dim).astype(jnp.float32) * (-2.0 * math.log(500000.0) / HEAD_SIZE)
    )
    angles = positions.astype(jnp.float32)[:, None] * inverse_freq[None, :]
    cos_table = jnp.cos(angles)[:, None, :]
    sin_table = jnp.sin(angles)[:, None, :]
    reshaped_rows = unshaped_rows.reshape(unshaped_rows.shape[0], KEY_VALUE_HEADS, HEAD_SIZE)
    first_half = reshaped_rows[..., :half_dim]
    second_half = reshaped_rows[..., half_dim:]
    transposed_rows = jnp.concatenate(
        [
            first_half * cos_table - second_half * sin_table,
            second_half * cos_table + first_half * sin_table,
        ],
        axis=-1,
    )
    return transposed_rows.reshape(unshaped_rows.shape[0], KEY_VALUE_HEADS * HEAD_SIZE)


def plain_body(queries, normed, key_weight_copies, value_weight_copies, owner):
    input_rows = normed[0]
    token_rows = input_rows.shape[0]
    owner_group = lax.dynamic_index_in_dim(owner, lax.axis_index("blk"), 0, keepdims=False)
    shards = (
        spread(key_weight_copies[0], "group", owner_group),
        spread(value_weight_copies[0], "group", owner_group),
    )
    pieces = [lax.all_gather(s, "blk", axis=0, tiled=True) for s in shards]
    key_raw = jnp.dot(input_rows, pieces[0], preferred_element_type=jnp.float32)
    value_raw = jnp.dot(input_rows, pieces[1], preferred_element_type=jnp.float32)
    positions = lax.axis_index("blk") * token_rows + jnp.arange(token_rows, dtype=jnp.int32)
    cache_keys = rotate(key_raw, positions).astype(jnp.bfloat16)
    cache_values = value_raw.astype(jnp.bfloat16)
    rep = QUERY_HEADS // KEY_VALUE_HEADS
    grid = queries[0].reshape(token_rows, KEY_VALUE_HEADS, rep, HEAD_SIZE)
    keys = lax.all_gather(cache_keys, "blk", axis=0, tiled=True)
    values = lax.all_gather(cache_values, "blk", axis=0, tiled=True)
    count = keys.shape[0]
    keys = keys.reshape(count, KEY_VALUE_HEADS, HEAD_SIZE)
    values = values.reshape(count, KEY_VALUE_HEADS, HEAD_SIZE)
    scores = jnp.einsum("lewc,jec->ewlj", grid, keys, preferred_element_type=jnp.float32)
    scores = scores * HEAD_SIZE ** (-0.5)
    allowed = jnp.arange(count, dtype=jnp.int32)[None, :] <= positions[:, None]
    scores = jnp.where(allowed, scores, -jnp.inf)
    probs = jnp.exp(scores - jnp.max(scores, axis=-1, keepdims=True))
    total = jnp.sum(probs, axis=-1)
    weighted = jnp.einsum(
        "lxbp,plj->lxbj", probs.astype(jnp.bfloat16), values, preferred_element_type=jnp.float32
    )
    attended = (weighted / total[..., None]).transpose(2, 0, 1, 3)
    attended = attended.reshape(token_rows, QUERY_HEADS * HEAD_SIZE).astype(jnp.bfloat16)
    return (cache_keys[None], cache_values[None], attended[None])


def kernel(
    dims, owner_ref, q_hbm, n_hbm, wk_hbm, wv_hbm, ck_ref, cv_ref, at_ref,
    qbuf, nbuf, ybuf, merged, zbuf, other, wb, proj, cos_t, sin_t, kvbuf, top, tot, acc,
    loc_sem, own_sem, y_send, y_recv, z_send, z_recv, n_send, n_recv, c_send, c_recv,
    gz_send, gy_send, gx_send, g_recv, p_send, p_recv, k_send, k_recv, f_send, f_recv,
):
    X, Z, Y = dims
    G = Z * Y
    T = q_hbm.shape[1]
    ch = wb.shape[2]
    half = HEAD_SIZE // 2
    g, b = lax.axis_index("group"), lax.axis_index("blk")
    z, y = g // Y, g % Y
    x, core = b // 2, b % 2
    twin = x * 2 + 1 - core

    def at(group, blk):
        return {"group": group, "blk": blk}

    def remote(src, dst, ss, rs, dev):
        return pltpu.make_async_remote_copy(
            src_ref=src, dst_ref=dst, send_sem=ss, recv_sem=rs, device_id=dev, device_id_type=MESH
        )

    z_others = [lax.rem(z + i, Z) for i in range(1, Z)]
    y_others = [lax.rem(y + i, Y) for i in range(1, Y)]
    x_others = [lax.rem(x + i, X) for i in range(1, X)]
    barrier = pltpu.get_barrier_semaphore()
    peers = [at(z * Y + yp, b) for yp in y_others]
    peers += [at(zp * Y + y, b) for zp in z_others]
    peers += [at(g, xp * 2 + core) for xp in x_others]
    peers += [at(g, twin)]
    for dev in peers:
        pl.semaphore_signal(barrier, inc=1, device_id=dev, device_id_type=MESH)

    z_order = z_others + [z]
    weights = (wk_hbm, wv_hbm)
    own = []
    for i, zp in enumerate(z_order):
        for k in range(2):
            rows = pl.ds(pl.multiple_of((zp * Y + y) * ch, ch), ch)
            cp = pltpu.make_async_copy(
                weights[k].at[0, rows], ybuf.at[y, zp, k], own_sem.at[i, k]
            )
            cp.start()
            own.append(cp)
    q_copy = pltpu.make_async_copy(q_hbm.at[0], qbuf, loc_sem.at[0])
    n_copy = pltpu.make_async_copy(n_hbm.at[0], nbuf.at[core], loc_sem.at[1])
    n_copy.start()
    q_copy.start()

    pl.semaphore_wait(barrier, len(peers))

    sends = []
    for zp in z_order:
        for yp in y_others:
            for k in range(2):
                rows = pl.ds(pl.multiple_of((zp * Y + yp) * ch, ch), ch)
                cp = remote(
                    weights[k].at[0, rows], ybuf.at[y, zp, k],
                    y_send.at[yp, zp, k], y_recv.at[y, zp, k], at(z * Y + yp, b),
                )
                cp.start()
                sends.append(cp)
    n_send_copy = remote(n_hbm.at[0], nbuf.at[core], n_send, n_recv, at(g, twin))
    n_send_copy.start()

    pos = (x * 2 * T + lax.broadcasted_iota(jnp.int32, (2 * T, HEAD_SIZE), 0)).astype(jnp.float32)
    lane = lax.broadcasted_iota(jnp.int32, (2 * T, HEAD_SIZE), 1)
    freq = jnp.exp((lane % half).astype(jnp.float32) * (-2.0 * math.log(500000.0) / HEAD_SIZE))
    angle = pos * freq
    cos_t[...] = jnp.cos(angle)
    sin_a = jnp.sin(angle)
    sin_t[...] = jnp.where(lane < half, -sin_a, sin_a)

    owner_group = owner_ref[b]
    owner_z, owner_y = owner_group // Y, owner_group % Y

    def pick(which, options):
        sel = options[0]
        for i in range(1, len(options)):
            sel = lax.select(which == i, options[i], sel)
        return sel

    for i, zp in enumerate(z_order):
        for k in range(2):
            own[2 * i + k].wait()
            for yp in y_others:
                pltpu.make_async_copy(
                    ybuf.at[yp, zp, k], ybuf.at[yp, zp, k], y_recv.at[yp, zp, k]
                ).wait()
        for k in range(2):
            sel = pick(owner_y, [ybuf[yy, zp, k] for yy in range(Y)])
            if i < Z - 1:
                merged[i, k] = sel
            else:
                zbuf[z, k] = sel
        if i < Z - 1:
            cp = remote(merged.at[i], zbuf.at[z], z_send.at[i], z_recv.at[z], at(zp * Y + y, b))
            cp.start()
            sends.append(cp)
    for zp in reversed(z_others):
        pltpu.make_async_copy(zbuf.at[zp], zbuf.at[zp], z_recv.at[zp]).wait()

    other[...] = pick(owner_z, [zbuf[zz, 1 - core] for zz in range(Z)])
    cp = remote(other, wb.at[b, g], c_send, c_recv, at(g, twin))
    cp.start()
    sends.append(cp)
    wb[b, g] = pick(owner_z, [zbuf[zz, core] for zz in range(Z)])
    pltpu.make_async_copy(wb.at[twin, g], wb.at[twin, g], c_recv).wait()

    def piece(xx, gg):
        return wb.at[pl.ds(2 * xx, 2), gg]

    def give(gg, ss, group, xx):
        cp = remote(piece(x, gg), piece(x, gg), ss, g_recv.at[x, gg], at(group, xx * 2 + core))
        cp.start()
        sends.append(cp)

    def arrived(xx, gg):
        pltpu.make_async_copy(piece(xx, gg), piece(xx, gg), g_recv.at[xx, gg]).wait()

    def to_x(gg):
        for xp in x_others:
            give(gg, gx_send.at[xp, gg], g, xp)

    def to_y(gg, zz):
        for yp in y_others:
            give(gg, gy_send.at[yp, zz], z * Y + yp, x)

    to_x(g)
    for zp in z_others:
        give(g, gz_send.at[zp], zp * Y + y, x)
    to_y(g, z)
    for zp in reversed(z_others):
        arrived(x, zp * Y + y)
        to_y(zp * Y + y, zp)
        to_x(zp * Y + y)
    for zp in [z] + z_others[::-1]:
        for yp in y_others:
            arrived(x, zp * Y + yp)
            to_x(zp * Y + yp)

    n_copy.wait()
    pltpu.make_async_copy(nbuf.at[1 - core], nbuf.at[1 - core], n_recv).wait()
    depth = 2 * G * ch
    cols = wb.shape[3]

    def product(xx):
        feats = pl.ds(pl.multiple_of(xx * depth, depth), depth)
        left = nbuf[:, :, feats].reshape(2 * T, depth)
        right = wb[pl.ds(2 * xx, 2)].reshape(depth, cols)
        return jnp.dot(left, right, preferred_element_type=jnp.float32)

    proj[...] = product(x)
    for xp in x_others:
        for zp in [z] + z_others[::-1]:
            arrived(xp, zp * Y + y)
        for zp in [z] + z_others[::-1]:
            for yp in y_others:
                arrived(xp, zp * Y + yp)
        proj[...] += product(xp)

    heads = [slice(h * HEAD_SIZE, (h + 1) * HEAD_SIZE) for h in range(KEY_VALUE_HEADS)]

    @pl.when(core == 0)
    def _():
        for hs in heads:
            part = proj[:, hs]
            turned = part * cos_t[...] + pltpu.roll(part, half, 1) * sin_t[...]
            kvbuf[0, x, :, hs] = turned.astype(jnp.bfloat16)

    @pl.when(core == 1)
    def _():
        kvbuf[1, x] = proj[...].astype(jnp.bfloat16)

    mine = kvbuf.at[core, x]
    for xp in range(X):
        @pl.when(xp > x)
        def _():
            remote(mine, mine, k_send.at[xp], k_recv.at[x], at(g, xp * 2 + core)).start()
    twin_copy = remote(mine, mine, p_send, p_recv, at(g, twin))
    twin_copy.start()
    q_copy.wait()
    theirs = kvbuf.at[1 - core, x]
    pltpu.make_async_copy(theirs, theirs, p_recv).wait()

    span = pl.ds(pl.multiple_of(core * T, T), T)
    ck_ref[0] = kvbuf[0, x, span, :]
    cv_ref[0] = kvbuf[1, x, span, :]

    rep = QUERY_HEADS // KEY_VALUE_HEADS
    scale = HEAD_SIZE ** (-0.5) * math.log2(math.e)

    def scored(h, xx):
        stacked = jnp.concatenate(
            [
                qbuf[:, (h * rep + j) * HEAD_SIZE : (h * rep + j + 1) * HEAD_SIZE]
                for j in range(rep)
            ],
            axis=0,
        )
        return lax.dot_general(
            stacked, kvbuf[0, xx, :, heads[h]], (((1,), (1,)), ((), ())),
            preferred_element_type=jnp.float32,
        )

    for h in range(KEY_VALUE_HEADS):
        s = scored(h, x)
        row = core * T + lax.rem(lax.broadcasted_iota(jnp.int32, s.shape, 0), T)
        s = jnp.where(lax.broadcasted_iota(jnp.int32, s.shape, 1) <= row, s, -jnp.inf)
        m = jnp.max(s, axis=1, keepdims=True)
        p = jnp.exp2((s - m) * scale)
        top[h] = m
        tot[h] = jnp.sum(p, axis=1, keepdims=True)
        acc[h] = jnp.dot(
            p.astype(jnp.bfloat16), kvbuf[1, x, :, heads[h]], preferred_element_type=jnp.float32
        )

    for xs in range(X):
        @pl.when(xs < x)
        def _():
            got = kvbuf.at[core, xs]
            pltpu.make_async_copy(got, got, k_recv.at[xs]).wait()
            remote(got, got, f_send.at[xs], f_recv.at[xs], at(g, twin)).start()
            rest = kvbuf.at[1 - core, xs]
            pltpu.make_async_copy(rest, rest, f_recv.at[xs]).wait()
            for h in range(KEY_VALUE_HEADS):
                s = scored(h, xs)
                old = top[h]
                m = jnp.maximum(old, jnp.max(s, axis=1, keepdims=True))
                fade = jnp.exp2((old - m) * scale)
                p = jnp.exp2((s - m) * scale)
                top[h] = m
                tot[h] = tot[h] * fade + jnp.sum(p, axis=1, keepdims=True)
                acc[h] = acc[h] * fade + jnp.dot(
                    p.astype(jnp.bfloat16), kvbuf[1, xs, :, heads[h]],
                    preferred_element_type=jnp.float32,
                )

    for h in range(KEY_VALUE_HEADS):
        done = (acc[h] / tot[h]).astype(jnp.bfloat16)
        for j in range(rep):
            at_ref[0, :, (h * rep + j) * HEAD_SIZE : (h * rep + j + 1) * HEAD_SIZE] = done[
                j * T : (j + 1) * T
            ]

    for cp in sends:
        cp.wait_send()
    n_send_copy.wait_send()
    twin_copy.wait_send()
    for xp in range(X):
        @pl.when(xp > x)
        def _():
            remote(mine, mine, k_send.at[xp], k_recv.at[x], at(g, xp * 2 + core)).wait_send()

        @pl.when(xp < x)
        def _():
            got = kvbuf.at[core, xp]
            remote(got, got, f_send.at[xp], f_recv.at[xp], at(g, twin)).wait_send()


def fused_body(dims, queries, normed, key_weight_copies, value_weight_copies, owner):
    X, Z, Y = dims
    G = Z * Y
    _, T, qcols = queries.shape
    feats = normed.shape[2]
    _, shard_rows, cols = key_weight_copies.shape
    ch = shard_rows // G
    bf, f32 = jnp.bfloat16, jnp.float32
    rep = QUERY_HEADS // KEY_VALUE_HEADS
    vm, dma = pltpu.VMEM, pltpu.SemaphoreType.DMA
    anyspace = pl.BlockSpec(memory_space=pl.ANY)
    vmem = pl.BlockSpec(memory_space=pltpu.VMEM)
    return pl.pallas_call(
        functools.partial(kernel, dims),
        out_shape=(
            jax.ShapeDtypeStruct((1, T, cols), bf),
            jax.ShapeDtypeStruct((1, T, cols), bf),
            jax.ShapeDtypeStruct((1, T, qcols), bf),
        ),
        in_specs=[pl.BlockSpec(memory_space=pltpu.SMEM)] + [anyspace] * 4,
        out_specs=(vmem, vmem, vmem),
        scratch_shapes=[
            vm((T, qcols), bf),
            vm((2, T, feats), bf),
            vm((Y, Z, 2, ch, cols), bf),
            vm((max(Z - 1, 1), 2, ch, cols), bf),
            vm((Z, 2, ch, cols), bf),
            vm((ch, cols), bf),
            vm((2 * X, G, ch, cols), bf),
            vm((2 * T, cols), f32),
            vm((2 * T, HEAD_SIZE), f32),
            vm((2 * T, HEAD_SIZE), f32),
            vm((2, X, 2 * T, cols), bf),
            vm((KEY_VALUE_HEADS, rep * T, 1), f32),
            vm((KEY_VALUE_HEADS, rep * T, 1), f32),
            vm((KEY_VALUE_HEADS, rep * T, HEAD_SIZE), f32),
            dma((2,)),
            dma((Z, 2)),
            dma((Y, Z, 2)),
            dma((Y, Z, 2)),
            dma((Z,)),
            dma((Z,)),
            dma,
            dma,
            dma,
            dma,
            dma((Z,)),
            dma((Y, Z)),
            dma((X, G)),
            dma((X, G)),
            dma,
            dma,
            dma((X,)),
            dma((X,)),
            dma((X,)),
            dma((X,)),
        ],
        compiler_params=pltpu.CompilerParams(
            collective_id=0, has_side_effects=True, vmem_limit_bytes=48 * 1024 * 1024
        ),
    )(owner, queries, normed, key_weight_copies, value_weight_copies)


def body(sizes, *args):
    n_blk, n_group = sizes
    shard_rows = args[2].shape[1]
    minor = 1
    while 2 * (2 * minor) ** 2 <= n_group:
        minor *= 2
    aligned = n_group % minor == 0 and shard_rows % (16 * n_group) == 0 and n_blk % 2 == 0
    if not aligned or args[0].shape[1] % 128:
        return plain_body(*args)
    return fused_body((n_blk // 2, n_group // minor, minor), *args)


def solution(mesh):
    split = P("group", "blk", None)
    return jax.shard_map(
        functools.partial(body, (mesh.shape["blk"], mesh.shape["group"])),
        mesh=mesh,
        in_specs=(split, split, split, split, P()),
        out_specs=(split, split, split),
        check_vma=False,
    )
```
